256 devices in a mesh: seq: 32 (over x, z), chan: 8 (over y, core).
Axes of the slice: x: 4, y: 4, z: 8, core: 2. Of those that a mesh axis runs over, the one named last changes fastest.
Arguments:
- x_in: bfloat16 [24576, 5120], P('seq', 'chan'), may hold values from -120 to 120
- z_gate: bfloat16 [24576, 5120], P('seq', 'chan'), may hold values from -6 to 6
- b_proj: bfloat16 [24576, 128], P('seq'), may hold values from -6 to 6
- c_proj: bfloat16 [24576, 128], P('seq'), may hold values from -6 to 6
- dt_step: float32 [80, 24576], P('chan', 'seq'), may hold values from 0 to 1
- a_log: float32 [80], P('chan'), may hold values from -0.35 to 0.35
- skip_gain: float32 [80], P('chan'), may hold values from 0.5 to 1.5
- norm_gain: float32 [5120], P('chan'), may hold values from 0.5 to 1.5
- out_weight: bfloat16 [2560, 5120], P('seq', 'chan'), may hold values from -0.078125 to 0.078125
- out_grad: bfloat16 [24576, 2560], P('seq'), may hold values from -6 to 6
Outputs:
- d_x: bfloat16 [24576, 5120], P('seq', 'chan')
- d_z: bfloat16 [24576, 5120], P('seq', 'chan')
- d_dt: float32 [80, 24576], P('chan', 'seq')
- d_out_weight: float32 [2560, 5120], P('seq', 'chan')
The draws below stay inside these ranges and needn't reach their ends.
All inputs are finite; a program needn't handle non-finite values.
Results may differ from the reference program's by a relative error of at most 0.005.
Values may be sent and summed in bfloat16 or wider, within the bound.
No kernel may reach another device: no remote copies, remote signals or barrier semaphores. Data moves between devices by JAX's collectives and lax.ppermute only.
A program may use at most 128 MiB of HBM per device.

```python
import math
from functools import partial
import jax
import jax.numpy as jnp
from jax import lax

D = 2560
SCAN_HEADS = 80
STATE = 128
GROUP = 256
TOK_DEV = 768
E = 5120
SEQUENCE_TOKENS = 24576


def draw_x_in(key, part):
    random_keys = jax.random.split(key, 3)
    channel = jnp.arange(E, dtype=jnp.float32) / E
    random_part = jnp.clip(jax.random.normal(random_keys[0], (SEQUENCE_TOKENS, E), jnp.float32), -6.0, 6.0)
    row_scale = jnp.exp(jax.random.uniform(random_keys[1], (SEQUENCE_TOKENS, 1), jnp.float32, math.log(0.3), math.log(3.0)))
    col_scale = jnp.exp(jax.random.uniform(random_keys[2], (1, E), jnp.float32, math.log(0.3), math.log(3.0))) * 1.7320508 ** channel[None, :]
    value_entries = random_part * row_scale * col_scale
    return value_entries.astype(jnp.bfloat16)


def draw_dt_step(key, part):
    random_keys = jax.random.split(key, 7)
    blocks = SEQUENCE_TOKENS // TOK_DEV
    slow_head = jax.random.uniform(random_keys[0], (SCAN_HEADS, 1), jnp.float32) < 0.5
    fast_rate = 7.0 / GROUP * jnp.exp(jax.random.uniform(random_keys[1], (SCAN_HEADS, 1), jnp.float32, math.log(0.75), math.log(1.15)))
    slow_rate = jnp.exp(jax.random.uniform(random_keys[2], (SCAN_HEADS, 1), jnp.float32, math.log(0.2), math.log(0.6))) / SEQUENCE_TOKENS
    base_rate = jnp.where(slow_head, slow_rate, fast_rate)
    device_factor = jnp.exp(jax.random.uniform(random_keys[3], (SCAN_HEADS, blocks), jnp.float32, math.log(0.5), math.log(2.0)))
    spread = jnp.repeat(device_factor, TOK_DEV, axis=1)
    jitter = jnp.exp(jax.random.uniform(random_keys[4], (SCAN_HEADS, SEQUENCE_TOKENS), jnp.float32, math.log(0.5), math.log(2.0)))
    value_entries = base_rate * spread * jitter
    spike_start = jax.random.randint(random_keys[5], (SCAN_HEADS, 2), 0, SEQUENCE_TOKENS)
    spike_length = jax.random.uniform(random_keys[6], (SCAN_HEADS, 2), jnp.float32, 0.25, 0.5)
    token_places = jnp.arange(SEQUENCE_TOKENS, dtype=jnp.int32)
    found_pairs = token_places[None, :, None] == spike_start[:, None, :]
    spike_list = jnp.max(jnp.where(found_pairs, spike_length[:, None, :], 0.0), axis=2)
    return jnp.maximum(value_entries, spike_list).astype(jnp.float32)


def strengthened(drawn, stream_key, source, target, blocks, factor):
    owner, partner = [(jnp.arange(drawn.shape[axis_at]) // (drawn.shape[axis_at] // blocks)).reshape([-1 if axis == axis_at else 1 for axis in range(drawn.ndim)]) for axis_at in (source, target)]
    chosen = jax.random.permutation(stream_key, blocks)[partner]
    strong = (owner == chosen) | (owner == (partner + blocks // 2) % blocks)
    return jnp.where(strong, factor * drawn, drawn)


def shard_levels(key, shape, cuts, least, largest):
    def one(dim, parts):
        steps = jax.random.uniform(jax.random.fold_in(jax.random.fold_in(key, 6), dim), (parts,), jnp.float32, least / len(cuts), largest / len(cuts))
        return jnp.repeat(jnp.exp(steps), shape[dim] // parts).reshape((-1,) + (1,) * (len(shape) - dim - 1))

    gain = one(*cuts[0])
    for cut in cuts[1:]:
        gain = gain * one(*cut)
    return gain


def bell_draw(key, dims, deviation, most, shards=(), kind=jnp.bfloat16):
    entries = deviation * jax.random.normal(key, dims, jnp.float32)
    if shards:
        entries = entries * shard_levels(key, dims, shards, -0.22, 0.18)
    return jnp.clip(entries, -most, most).astype(kind)


def gaussian_with(rng, dims, scale, most, shards, heavy, held_as=jnp.bfloat16):
    drawn = scale * jax.random.normal(rng, dims, jnp.float32)
    if shards:
        drawn = drawn * shard_levels(rng, dims, shards, -0.22, 0.18)
    return jnp.clip(strengthened(drawn, jax.random.fold_in(rng, 3), *heavy), -most, most).astype(held_as)


def setup_inputs(seed: int = 0) -> dict:
    arg_keys = jax.random.split(jax.random.key(seed), 11)
    return {
        "x_in": draw_x_in(jax.random.fold_in(arg_keys[10], 71), 0),
        "z_gate": bell_draw(arg_keys[1], (SEQUENCE_TOKENS, E), 1.0, 6.0, ((0, 32), (1, 8))),
        "b_proj": bell_draw(arg_keys[2], (SEQUENCE_TOKENS, STATE), 1.0, 6.0, ((0, 32),)),
        "c_proj": bell_draw(arg_keys[3], (SEQUENCE_TOKENS, STATE), 1.0, 6.0, ((0, 32),)),
        "dt_step": draw_dt_step(jax.random.fold_in(arg_keys[10], 71), 0),
        "a_log": jnp.clip(jax.random.uniform(arg_keys[5], (SCAN_HEADS,), jnp.float32, -0.35, 0.35) * shard_levels(arg_keys[5], (SCAN_HEADS,), ((0, 8),), -0.4, 0.0), -0.35, 0.35),
        "skip_gain": jnp.clip(1.0 + 0.1 * jax.random.normal(arg_keys[6], (SCAN_HEADS,), jnp.float32), 0.5, 1.5),
        "norm_gain": jnp.clip(1.0 + 0.1 * jax.random.normal(arg_keys[7], (E,), jnp.float32), 0.5, 1.5),
        "out_weight": bell_draw(arg_keys[8], (D, E), E ** -0.5, 0.078125, ((0, 32), (1, 8))),
        "out_grad": gaussian_with(arg_keys[9], (SEQUENCE_TOKENS, D), 1.0, 6.0, ((0, 32),), (0, 1, 32, 2.75)),
    }


norm_eps = 1e-05
highest = lax.Precision.HIGHEST

def group_step(state_in, pieces, decay_rates, skip_gain):
    x_part, dt_part, b_part, c_part = pieces
    log_decay = jnp.cumsum(-decay_rates[:, None] * dt_part, axis=1)
    length = dt_part.shape[1]
    row_ids = lax.broadcasted_iota(jnp.int32, (length, length), 0)
    col_ids = lax.broadcasted_iota(jnp.int32, (length, length), 1)
    causal = (row_ids >= col_ids)[None]
    log_gap = jnp.where(causal, log_decay[:, :, None] - log_decay[:, None, :], 0.0)
    decay_mat = jnp.where(causal, jnp.exp(log_gap), 0.0)
    affinity = jnp.dot(c_part, b_part.T, precision=highest)
    weighted = x_part * jnp.transpose(dt_part)[:, :, None]
    within = jnp.einsum('hts,shp->thp', decay_mat * affinity[None], weighted, precision=highest)
    carried = jnp.transpose(jnp.exp(log_decay))[:, :, None] * jnp.einsum('tn,hpn->thp', c_part, state_in, precision=highest)
    output = within + carried + skip_gain[None, :, None] * x_part
    to_end = jnp.exp(log_decay[:, -1:] - log_decay)
    update = jnp.einsum('shp,hs,sn->hpn', weighted, to_end, b_part, precision=highest)
    state_out = jnp.exp(log_decay[:, -1])[:, None, None] * state_in + update
    return (state_out, output)

def ssd_local(x_vals, dt_vals, b_vals, c_vals, decay_rates, skip_gain, state_in):
    length, head_count, head_size = x_vals.shape
    blocks = length // GROUP
    x_blocks = x_vals.reshape(blocks, GROUP, head_count, head_size)
    dt_blocks = jnp.transpose(dt_vals.reshape(head_count, blocks, GROUP), (1, 0, 2))
    b_blocks = b_vals.reshape(blocks, GROUP, -1)
    c_blocks = c_vals.reshape(blocks, GROUP, -1)
    stepper = jax.checkpoint(partial(group_step, decay_rates=decay_rates, skip_gain=skip_gain))
    state_out, outputs = lax.scan(stepper, state_in, (x_blocks, dt_blocks, b_blocks, c_blocks))
    return (outputs.reshape(length, head_count, head_size), state_out)

def reference(x_in, z_gate, b_proj, c_proj, dt_step, a_log, skip_gain, norm_gain, out_weight, out_grad):
    total, width = x_in.shape
    head_count = a_log.shape[0]
    head_size = width // head_count
    decay_rates = jnp.exp(a_log)
    b_vals = b_proj.astype(jnp.float32)
    c_vals = c_proj.astype(jnp.float32)
    zero_state = jnp.zeros((head_count, head_size, b_vals.shape[1]), jnp.float32)

    def forward(x_arg, z_arg, dt_arg):
        x_vals = x_arg.astype(jnp.float32).reshape(total, head_count, head_size)
        y_vals, state_end = ssd_local(x_vals, dt_arg, b_vals, c_vals, decay_rates, skip_gain, zero_state)
        gated_y = y_vals.reshape(total, width) * jax.nn.silu(z_arg.astype(jnp.float32))
        scale_inv = lax.rsqrt(lax.optimization_barrier(jnp.mean(gated_y * gated_y, axis=1, keepdims=True)) + norm_eps)
        return (gated_y * scale_inv * norm_gain).astype(jnp.bfloat16)
    normed, pull_back = jax.vjp(forward, x_in, z_gate, dt_step)
    grad_norm = jnp.dot(out_grad, out_weight, preferred_element_type=jnp.float32).astype(jnp.bfloat16)
    weight_grad = lax.dot_general(out_grad, normed, (((0,), (0,)), ((), ())), preferred_element_type=jnp.float32)
    grad_x, grad_z, grad_dt = pull_back(grad_norm)
    return (grad_x, grad_z, grad_dt, weight_grad)
```

```python
import functools

import jax
import jax.numpy as jnp
from jax import lax
from jax.experimental import pallas as pl
from jax.experimental.pallas import tpu as pltpu
from jax.sharding import Mesh
from jax.sharding import PartitionSpec as P

SEQ = ("seq_0", "seq_1")
Q = 128
HEAD = 64
EPS = 1e-05
F32 = jnp.float32
BF16 = jnp.bfloat16
HI = lax.Precision.HIGHEST
NN = (((1,), (0,)), ((), ()))
NT = (((1,), (1,)), ((), ()))


def mm(a, b, dims=NN):
    return lax.dot_general(a, b, dims, preferred_element_type=F32)


def mm_exact(a, b, dims=NN):
    return lax.dot_general(a, b, dims, precision=HI, preferred_element_type=F32)


def split_mm(a, b, dims):
    high = b.astype(BF16)
    low = (b - high.astype(F32)).astype(BF16)
    return mm(a, high, dims) + mm(a, low, dims)


def iota(shape, dim):
    return lax.broadcasted_iota(jnp.int32, shape, dim)


def head_sum_matrix(width):
    return (iota((16, width), 1) // HEAD == iota((16, width), 0)).astype(BF16)


def log_decays(dt, a_log):
    return -jnp.exp(a_log) * dt


def run_rows(la):
    upper = (iota((Q, Q), 0) <= iota((Q, Q), 1)).astype(F32)
    return mm_exact(la, upper)


def run_cols(la):
    lower = (iota((Q, Q), 0) >= iota((Q, Q), 1)).astype(F32)
    return mm_exact(lower, la, NT)


def pair_row(column, j):
    lane = iota((1, 2 * HEAD), 1)
    return jnp.where(lane < HEAD, column[2 * j : 2 * j + 1, :], column[2 * j + 1 : 2 * j + 2, :])


def halves(pair):
    lane = iota(pair.shape, 1)
    zero = jnp.zeros_like(pair)
    return (jnp.where(lane < HEAD, pair, zero), jnp.where(lane >= HEAD, pair, zero))


def pair_slice(j):
    return slice(2 * HEAD * j, 2 * HEAD * (j + 1))


def sigmoid(v):
    return 1.0 / (1.0 + jnp.exp(-v))


def outer_state(left_t, weights, right, j):
    lhs = jnp.concatenate(
        [(left_t * weights[h : h + 1, :]).astype(BF16) for h in (2 * j, 2 * j + 1)], axis=1
    )
    first, second = halves(right)
    return mm(lhs, jnp.concatenate([first, second], axis=0).astype(BF16))


def state_kernel(dt_ref, alog_ref, x_ref, b_ref, inc_ref, state_ref, ldev_ref):
    @pl.when(pl.program_id(0) == 0)
    def _():
        state_ref[...] = jnp.zeros_like(state_ref)
        ldev_ref[...] = jnp.zeros_like(ldev_ref)

    dt = dt_ref[...]
    run = run_rows(log_decays(dt, alog_ref[...]))
    total = run[:, Q - 1 :]
    weights = jnp.exp(total - run) * dt
    b_t = jnp.transpose(b_ref[...].astype(F32))
    for j in range(dt.shape[0] // 2):
        cols = pair_slice(j)
        inc = outer_state(b_t, weights, x_ref[:, cols].astype(F32), j)
        inc_ref[0, :, cols] = inc
        row = pair_row(total, j)
        state_ref[:, cols] = jnp.exp(row) * state_ref[:, cols] + inc
        ldev_ref[:, cols] += row


def y_kernel(
    dt_ref, alog_ref, x_ref, b_ref, c_ref, inc_ref, in_ref, z_ref, skip_ref,
    y_ref, end_ref, sq_ref, state,
):
    @pl.when(pl.program_id(0) == 0)
    def _():
        state[...] = in_ref[...]

    dt = dt_ref[...]
    la = log_decays(dt, alog_ref[...])
    run, cols_run = run_rows(la), run_cols(la)
    total = run[:, Q - 1 :]
    c_part = c_ref[...]
    c_vals = c_part.astype(F32)
    affinity = mm(c_part, b_ref[...], NT)
    causal = iota((Q, Q), 0) >= iota((Q, Q), 1)
    squares = jnp.zeros((Q, 2 * HEAD), F32)
    for j in range(dt.shape[0] // 2):
        cols = pair_slice(j)
        x_pair = x_ref[:, cols]
        x_first, x_second = halves(x_pair.astype(F32))
        before = state[:, cols]
        s_first, s_second = halves(before)
        left = []
        for h in (2 * j, 2 * j + 1):
            at = jnp.broadcast_to(cols_run[:, h : h + 1], (Q, Q))
            decay = jnp.exp(jnp.where(causal, at - run[h : h + 1, :], -1e30))
            left.append((decay * affinity * dt[h : h + 1, :]).astype(BF16))
            left.append((jnp.exp(at[:, : c_vals.shape[1]]) * c_vals).astype(BF16))
        lhs = jnp.concatenate(left, axis=1)
        rhs = jnp.concatenate([x_first, s_first, x_second, s_second], axis=0).astype(BF16)
        y_pair = mm(lhs, rhs)
        y_ref[:, cols] = y_pair
        after = jnp.exp(pair_row(total, j)) * before + inc_ref[0, :, cols]
        end_ref[0, :, cols] = after
        state[:, cols] = after
        z = z_ref[:, cols].astype(F32)
        gated = (y_pair + skip_ref[:, cols] * x_pair.astype(F32)) * (z * sigmoid(z))
        squares += gated * gated
    sq_ref[...] = split_mm(jnp.ones((8, 2 * HEAD), BF16), squares, NT)[:1]


def token_column(row):
    eye = (iota((Q, Q), 0) == iota((Q, Q), 1)).astype(F32)
    return mm_exact(eye, jnp.broadcast_to(row, (8, Q)), NT)[:, :1]


def gate_kernel(
    full_width,
    dt_ref, alog_ref, c_ref, y_ref, x_ref, z_ref, g_ref, skip_ref, gain_ref, sq_ref, dot_ref,
    gy_ref, dz_ref, inc_ref, state_ref,
):
    @pl.when(pl.program_id(0) == 0)
    def _():
        state_ref[...] = jnp.zeros_like(state_ref)

    dt = dt_ref[...]
    run = run_rows(log_decays(dt, alog_ref[...]))
    total = run[:, Q - 1 :]
    grow = jnp.exp(run)
    c_t = jnp.transpose(c_ref[...].astype(F32))
    inverse = lax.rsqrt(sq_ref[...] / full_width + EPS)
    inv_col = token_column(inverse)
    dot_col = token_column(inverse * inverse * inverse * dot_ref[...] / full_width)
    for j in range(dt.shape[0] // 2):
        cols = pair_slice(j)
        z = z_ref[:, cols].astype(F32)
        sig = sigmoid(z)
        act = z * sig
        y = y_ref[:, cols] + skip_ref[:, cols] * x_ref[:, cols].astype(F32)
        scaled = g_ref[:, cols].astype(F32) * gain_ref[:, cols]
        grad_gated = inv_col * scaled - (y * act) * dot_col
        dz_ref[:, cols] = (grad_gated * y * sig * (1.0 + z * (1.0 - sig))).astype(BF16)
        gy = (grad_gated * act).astype(BF16)
        gy_ref[:, cols] = gy
        inc = outer_state(c_t, grow, gy.astype(F32), j)
        inc_ref[0, :, cols] = inc
        state_ref[:, cols] = jnp.exp(pair_row(total, j)) * state_ref[:, cols] + inc


def grad_kernel(
    dt_ref, alog_ref, x_ref, b_ref, c_ref, y_ref, gy_ref, inc_ref, end_ref, in_ref, skip_ref,
    dx_ref, ddt_ref, state, prod,
):
    @pl.when(pl.program_id(0) == 0)
    def _():
        state[...] = in_ref[...]

    dt = dt_ref[...]
    heads = dt.shape[0]
    width = heads * HEAD
    a_log = alog_ref[...]
    la = log_decays(dt, a_log)
    run, cols_run = run_rows(la), run_cols(la)
    total = run[:, Q - 1 :]
    eye = (iota((Q, Q), 0) == iota((Q, Q), 1)).astype(F32)
    cols_dt = mm_exact(eye, dt, NT)
    b_part = b_ref[...]
    b_vals = b_part.astype(F32)
    affinity = mm(b_part, c_ref[...], NT)
    later = iota((Q, Q), 1) >= iota((Q, Q), 0)
    lane = iota((Q, 2 * HEAD), 1)
    for j in range(heads // 2):
        cols = pair_slice(j)
        gy = gy_ref[:, cols].astype(F32)
        g_first, g_second = halves(gy)
        after = state[:, cols]
        s_first, s_second = halves(after)
        left = []
        for h in (2 * j, 2 * j + 1):
            at = jnp.broadcast_to(cols_run[:, h : h + 1], (Q, Q))
            decay = jnp.exp(jnp.where(later, run[h : h + 1, :] - at, -1e30))
            left.append((decay * affinity).astype(BF16))
            tail = total[h : h + 1, :] - at[:, : b_vals.shape[1]]
            left.append((jnp.exp(tail) * b_vals).astype(BF16))
        lhs = jnp.concatenate(left, axis=1)
        rhs = jnp.concatenate([g_first, s_first, g_second, s_second], axis=0).astype(BF16)
        grad_in = mm(lhs, rhs)
        step = jnp.where(
            lane < HEAD, cols_dt[:, 2 * j : 2 * j + 1], cols_dt[:, 2 * j + 1 : 2 * j + 2]
        )
        scaled = step * grad_in
        dx_ref[:, cols] = (scaled + skip_ref[:, cols] * gy).astype(BF16)
        x = x_ref[:, cols].astype(F32)
        prod[0, :, cols] = x * grad_in
        prod[1, :, cols] = gy * y_ref[:, cols] - x * scaled
        crossing = (after * end_ref[0, :, cols]).reshape(-1, 8, 2 * HEAD)
        prod[2, :8, cols] = jnp.sum(crossing, axis=0)
        state[:, cols] = jnp.exp(pair_row(total, j)) * after + inc_ref[0, :, cols]
    heads_of = head_sum_matrix(width)
    direct = split_mm(heads_of, prod[0], NT)[:heads]
    change = split_mm(heads_of, prod[1], NT)[:heads]
    cross = jnp.sum(split_mm(heads_of, prod[2, :8, :], NT), axis=1, keepdims=True)[:heads]
    lower = (iota((Q, Q), 0) >= iota((Q, Q), 1)).astype(F32)
    grad_la = mm_exact(change, lower) + cross
    ddt_ref[...] = direct - jnp.exp(a_log) * grad_la


def scan_kernel(pair_in, reverse, in_ref, decay_ref, out_ref):
    peers = in_ref.shape[0]
    low = iota((8, in_ref.shape[2]), 0) < 4
    running = jnp.zeros(in_ref.shape[1:], F32)
    for k in reversed(range(peers)) if reverse else range(peers):
        high = running.astype(BF16).astype(F32)
        rest = pltpu.roll(running - high, 4, 0)
        out_ref[k] = jnp.where(low, high, rest).astype(BF16)
        part = in_ref[k].astype(F32)
        if pair_in:
            part = part + pltpu.roll(part, 4, 0)
        running = decay_ref[k] * running + part


def call(kernel, grid, in_specs, out_specs, out_shape, scratch=(), flops=2e9, name=None):
    return pl.pallas_call(
        kernel,
        grid=grid,
        in_specs=in_specs,
        out_specs=out_specs,
        out_shape=out_shape,
        scratch_shapes=scratch,
        name=name,
        compiler_params=pltpu.CompilerParams(
            dimension_semantics=("arbitrary",) * len(grid), vmem_limit_bytes=40 << 20
        ),
        cost_estimate=pl.CostEstimate(
            flops=int(flops), bytes_accessed=8 << 20, transcendentals=0
        ),
    )


def spread(state):
    peers = lax.axis_size(SEQ[0]) * lax.axis_size(SEQ[1])
    return state.reshape(peers, -1, state.shape[1])


def shards(
    x_in, z_gate, b_proj, c_proj, dt_step, a_log, skip_gain, norm_gain, out_weight, out_grad
):
    length, width = x_in.shape
    heads = a_log.shape[0]
    blocks = length // Q
    nstate = b_proj.shape[1]
    full_width = width * lax.axis_size("chan")
    alog = a_log[:, None]
    skip_row = jnp.repeat(skip_gain, HEAD)[None]
    gain_row = norm_gain[None]

    def shape(*dims, kind=F32):
        return jax.ShapeDtypeStruct(dims, kind)

    def specs(order):
        return dict(
            dt=pl.BlockSpec((heads, Q), lambda i: (0, order(i))),
            alog=pl.BlockSpec((heads, 1), lambda i: (0, 0)),
            wide=pl.BlockSpec((Q, width), lambda i: (order(i), 0)),
            bc=pl.BlockSpec((Q, nstate), lambda i: (order(i), 0)),
            inc=pl.BlockSpec((1, nstate, width), lambda i: (order(i), 0, 0)),
            state=pl.BlockSpec((nstate, width), lambda i: (0, 0)),
            row=pl.BlockSpec((1, width), lambda i: (0, 0)),
            tok=pl.BlockSpec((1, Q), lambda i: (0, order(i))),
        )

    up = specs(lambda i: i)
    down = specs(lambda i: blocks - 1 - i)

    inc, own_state, log_device = call(
        state_kernel,
        (blocks,),
        [up["dt"], up["alog"], up["wide"], up["bc"]],
        [up["inc"], up["state"], up["row"]],
        [shape(blocks, nstate, width), shape(nstate, width), shape(1, width)],
        name="own_state",
    )(dt_step, alog, x_in, b_proj)

    parts = spread(own_state)
    peers = parts.shape[0]
    d1 = log_device.astype(BF16)
    d2 = (log_device - d1.astype(F32)).astype(BF16)
    d3 = (log_device - d1.astype(F32) - d2.astype(F32)).astype(BF16)
    logs = jnp.concatenate([d1, d2, d3, jnp.zeros_like(d1)], axis=0)
    payload = jnp.concatenate(
        [parts.astype(BF16), jnp.broadcast_to(logs[None], (peers, 4, width))], axis=1
    )
    arrived = lax.all_to_all(payload, SEQ, 0, 0, tiled=True)
    decays = jnp.exp(jnp.sum(arrived[:, 4:7].astype(F32), axis=1, keepdims=True))

    def scanned(arrived, pair_in, reverse, name):
        whole = pl.BlockSpec((peers, 8, width), lambda i: (0, 0, 0))
        return call(
            functools.partial(scan_kernel, pair_in, reverse),
            (1,),
            [whole, pl.BlockSpec((peers, 1, width), lambda i: (0, 0, 0))],
            whole,
            shape(peers, 8, width, kind=BF16),
            name=name,
        )(arrived, decays)

    def entering(scanned_parts):
        back = lax.all_to_all(scanned_parts, SEQ, 0, 0, tiled=True).astype(F32)
        return (back[:, :4] + back[:, 4:]).reshape(nstate, width)

    state_in = entering(scanned(arrived, False, False, "scan_up"))

    y, ends, squares = call(
        y_kernel,
        (blocks,),
        [up["dt"], up["alog"], up["wide"], up["bc"], up["bc"], up["inc"], up["state"],
         up["wide"], up["row"]],
        [up["wide"], up["inc"], up["tok"]],
        [shape(length, width), shape(blocks, nstate, width), shape(1, length)],
        [pltpu.VMEM((nstate, width), F32)],
        name="y",
    )(dt_step, alog, x_in, b_proj, c_proj, inc, state_in, z_gate, skip_row)

    def chan_sum(value):
        size = lax.axis_size("chan")
        copies = jnp.broadcast_to(value[None], (size, *value.shape))
        return jnp.sum(lax.all_to_all(copies, "chan", 0, 0, tiled=True), axis=0)

    square_sum = chan_sum(squares)
    z_vals = z_gate.astype(F32)
    gated = (y + skip_row * x_in.astype(F32)) * (z_vals * sigmoid(z_vals))
    inverse = lax.rsqrt(square_sum[0] / full_width + EPS)
    normed = (gated * inverse[:, None] * gain_row).astype(BF16)
    partial = lax.dot_general(
        out_grad, normed, (((0,), (0,)), ((), ())), preferred_element_type=F32
    ).astype(BF16)

    weight = out_weight
    for axis in SEQ:
        weight = lax.all_gather(weight, axis)
    weight = jnp.swapaxes(weight, 0, 1).reshape(-1, width)
    grad_norm = mm(out_grad, weight).astype(BF16)
    dots = jnp.sum(gated * (grad_norm.astype(F32) * gain_row), axis=1)[None]
    dot_sum = chan_sum(dots)

    x_peers, z_peers = lax.axis_size(SEQ[0]), lax.axis_size(SEQ[1])
    held = partial.reshape(x_peers, -1, width)
    held = lax.all_to_all(held, SEQ[0], 0, 0, tiled=True).astype(F32).sum(0).astype(BF16)
    held = held.reshape(z_peers, -1, width)
    weight_grad = lax.all_to_all(held, SEQ[1], 0, 0, tiled=True).astype(F32).sum(0)

    grad_y, grad_z, grad_inc, own_grad = call(
        functools.partial(gate_kernel, float(full_width)),
        (blocks,),
        [down["dt"], down["alog"], down["bc"], down["wide"], down["wide"], down["wide"],
         down["wide"], down["row"], down["row"], down["tok"], down["tok"]],
        [down["wide"], down["wide"], down["inc"], down["state"]],
        [shape(length, width, kind=BF16), shape(length, width, kind=BF16),
         shape(blocks, nstate, width), shape(nstate, width)],
        name="gate",
    )(dt_step, alog, c_proj, y, x_in, z_gate, grad_norm, skip_row, gain_row, square_sum, dot_sum)

    parts = spread(own_grad)
    high = parts.astype(BF16)
    payload = jnp.concatenate([high, (parts - high.astype(F32)).astype(BF16)], axis=1)
    arrived = lax.all_to_all(payload, SEQ, 0, 0, tiled=True)
    grad_out = entering(scanned(arrived, True, True, "scan_down"))

    grad_x, grad_dt = call(
        grad_kernel,
        (blocks,),
        [down["dt"], down["alog"], down["wide"], down["bc"], down["bc"], down["wide"],
         down["wide"], down["inc"], down["inc"], down["state"], down["row"]],
        [down["wide"], down["dt"]],
        [shape(length, width, kind=BF16), shape(heads, length)],
        [pltpu.VMEM((nstate, width), F32), pltpu.VMEM((3, Q, width), F32)],
        name="grad",
    )(dt_step, alog, x_in, b_proj, c_proj, y, grad_y, grad_inc, ends, grad_out, skip_row)
    return (grad_x, grad_z, grad_dt, weight_grad)


def solution(mesh):
    z_axis = 8 if mesh.shape["seq"] % 8 == 0 else 2
    torus = Mesh(
        mesh.devices.reshape(-1, z_axis, mesh.shape["chan"]), ("seq_0", "seq_1", "chan")
    )
    return jax.shard_map(
        shards,
        mesh=torus,
        in_specs=(
            P(SEQ, "chan"),
            P(SEQ, "chan"),
            P(SEQ, None),
            P(SEQ, None),
            P("chan", SEQ),
            P("chan"),
            P("chan"),
            P("chan"),
            P(SEQ, "chan"),
            P(SEQ, None),
        ),
        out_specs=(P(SEQ, "chan"), P(SEQ, "chan"), P("chan", SEQ), P(SEQ, "chan")),
        check_vma=False,
    )
```

```python
import functools

import jax
import jax.numpy as jnp
from jax import lax
from jax.experimental import pallas as pl
from jax.experimental.pallas import tpu as pltpu
from jax.sharding import Mesh
from jax.sharding import PartitionSpec as P

SEQ = ("seq_0", "seq_1")
Q = 128
HEAD = 64
EPS = 1e-05
F32 = jnp.float32
BF16 = jnp.bfloat16
HI = lax.Precision.HIGHEST
NN = (((1,), (0,)), ((), ()))
NT = (((1,), (1,)), ((), ()))


def mm(a, b, dims=NN):
    return lax.dot_general(a, b, dims, preferred_element_type=F32)


def mm_exact(a, b, dims=NN):
    return lax.dot_general(a, b, dims, precision=HI, preferred_element_type=F32)


def split_mm(a, b, dims):
    high = b.astype(BF16)
    low = (b - high.astype(F32)).astype(BF16)
    return mm(a, high, dims) + mm(a, low, dims)


def iota(shape, dim):
    return lax.broadcasted_iota(jnp.int32, shape, dim)


def head_sum_matrix(width):
    return (iota((16, width), 1) // HEAD == iota((16, width), 0)).astype(BF16)


def rates(a_log):
    heads = a_log.shape[1]
    square = (heads, heads)
    picked = jnp.where(iota(square, 0) == iota(square, 1), jnp.broadcast_to(a_log, square), 0.0)
    return jnp.exp(jnp.sum(picked, axis=1, keepdims=True))


def log_decays(dt, a_log):
    return -rates(a_log) * dt


ROWS = 16


def block_runs(la, dt, blocks, rows_ref, cols_ref):
    pad = jnp.zeros((ROWS - la.shape[0], Q), F32)
    stack = jnp.concatenate(
        [p for i in range(blocks) for p in (la[:, i * Q : (i + 1) * Q], pad)], axis=0
    )
    steps = jnp.concatenate(
        [p for i in range(blocks) for p in (dt[:, i * Q : (i + 1) * Q], pad)], axis=0
    )
    upper = (iota((Q, Q), 0) <= iota((Q, Q), 1)).astype(F32)
    runs = mm_exact(stack, upper)
    rows_ref[...] = runs
    fill = jnp.zeros((Q - ROWS * blocks, Q), F32)
    runs_t = jnp.transpose(jnp.concatenate([runs, fill], axis=0))
    steps_t = jnp.transpose(jnp.concatenate([steps, fill], axis=0))
    for i in range(blocks):
        at = slice(ROWS * i, ROWS * (i + 1))
        cols_ref[i * Q : (i + 1) * Q, :ROWS] = runs_t[:, at]
        cols_ref[i * Q : (i + 1) * Q, ROWS : 2 * ROWS] = steps_t[:, at]


def pair_row(column, j):
    lane = iota((1, 2 * HEAD), 1)
    return jnp.where(lane < HEAD, column[2 * j : 2 * j + 1, :], column[2 * j + 1 : 2 * j + 2, :])


def halves(pair):
    lane = iota(pair.shape, 1)
    zero = jnp.zeros_like(pair)
    return (jnp.where(lane < HEAD, pair, zero), jnp.where(lane >= HEAD, pair, zero))


def pair_slice(j):
    return slice(2 * HEAD * j, 2 * HEAD * (j + 1))


def sigmoid(v):
    return 1.0 / (1.0 + jnp.exp(-v))


def outer_state(left_t, weights, right, j):
    lhs = jnp.concatenate(
        [(left_t * weights[h : h + 1, :]).astype(BF16) for h in (2 * j, 2 * j + 1)], axis=1
    )
    first, second = halves(right)
    return mm(lhs, jnp.concatenate([first, second], axis=0).astype(BF16))


def pack_parts(parts_ref, state_ref, extra):
    tiles = [pair_slice(j) for j in range(state_ref.shape[1] // (2 * HEAD))]
    top = iota((8, 2 * HEAD), 0) < 4
    for g in range(state_ref.shape[0] // 8):
        rows = [state_ref[8 * g : 8 * g + 8, t] for t in tiles]
        swapped = [pltpu.roll(r, 4, 0) for r in rows]
        if len(rows) % 2:
            rows.append(extra)
            swapped.append(extra)
        for v in range(len(rows) // 2):
            at = slice(8 * v, 8 * v + 8)
            parts_ref[2 * g, at, :] = jnp.where(top, rows[2 * v], swapped[2 * v + 1]).astype(BF16)
            parts_ref[2 * g + 1, at, :] = jnp.where(top, swapped[2 * v], rows[2 * v + 1]).astype(
                BF16
            )


def unpack_parts(state_ref, parts_ref):
    top = iota((8, 2 * HEAD), 0) < 4
    for g in range(state_ref.shape[0] // 8):
        for j in range(state_ref.shape[1] // (2 * HEAD)):
            at = slice(8 * (j // 2), 8 * (j // 2) + 8)
            first, second = parts_ref[2 * g, at, :], parts_ref[2 * g + 1, at, :]
            first, second = first.astype(F32), second.astype(F32)
            if j % 2 == 0:
                rows = jnp.where(top, first, pltpu.roll(second, 4, 0))
            else:
                rows = jnp.where(top, pltpu.roll(first, 4, 0), second)
            state_ref[8 * g : 8 * g + 8, pair_slice(j)] = rows


def state_kernel(
    blocks, step, last, at, dt_ref, alog_ref, x_ref, b_ref, inc_ref, parts_ref, rows_ref, cols_ref, state, ldev,
):
    heads = dt_ref.shape[0]

    @pl.when(step == 0)
    def _():
        state[...] = jnp.zeros_like(state)
        dt = dt_ref[...]
        block_runs(log_decays(dt, alog_ref[...]), dt, blocks, rows_ref, cols_ref)
        ldev[...] = jnp.zeros_like(ldev)

    run = rows_ref[pl.ds(pl.multiple_of(at * ROWS, ROWS), ROWS), :]
    dt = dt_ref[:, pl.ds(pl.multiple_of(at * Q, Q), Q)]
    total = run[:, Q - 1 :]
    weights = jnp.exp(total[:heads] - run[:heads]) * dt
    ldev[...] += jnp.broadcast_to(total, ldev.shape)
    b_t = jnp.transpose(b_ref[...].astype(F32))
    for j in range(heads // 2):
        cols = pair_slice(j)
        inc = outer_state(b_t, weights, x_ref[:, cols].astype(F32), j)
        inc_ref[0, :, cols] = inc
        state[:, cols] = jnp.exp(pair_row(total, j)) * state[:, cols] + inc

    @pl.when(last)
    def _():
        picked = jnp.where(iota((ROWS, Q), 0) == iota((ROWS, Q), 1), ldev[...], 0.0)
        logs = jnp.broadcast_to(jnp.sum(picked, axis=0, keepdims=True), (8, Q))
        first = logs.astype(BF16).astype(F32)
        second = (logs - first).astype(BF16).astype(F32)
        row = iota((8, Q), 0) % 4
        rest = jnp.where(row == 2, logs - first - second, 0.0)
        pack_parts(
            parts_ref, state, jnp.where(row == 0, first, jnp.where(row == 1, second, rest))
        )


def pair_cols(columns, j):
    lane = iota((Q, 2 * HEAD), 1)
    return jnp.where(lane < HEAD, columns[:, 2 * j : 2 * j + 1], columns[:, 2 * j + 1 : 2 * j + 2])


def near_product(matrices, right):
    lhs = jnp.concatenate([m.astype(BF16) for m in matrices], axis=1)
    return mm(lhs, jnp.concatenate(halves(right), axis=0).astype(BF16))


def far_product(maps, state):
    high = state.astype(BF16)
    low = (state - high.astype(F32)).astype(BF16)
    return mm(jnp.concatenate([maps, maps], axis=1), jnp.concatenate([high, low], axis=0))


def near_kernel(
    step, last, at, dt_ref, rows_ref, cols_ref, x_ref, b_ref, c_ref, near_ref):
    dt = dt_ref[...]
    run, cols_run = rows_ref[...], cols_ref[...]
    affinity = mm(c_ref[...], b_ref[...], NT)
    causal = iota((Q, Q), 0) >= iota((Q, Q), 1)
    for j in range(dt.shape[0] // 2):
        cols = pair_slice(j)
        mats = []
        for h in (2 * j, 2 * j + 1):
            at = jnp.broadcast_to(cols_run[:, h : h + 1], (Q, Q))
            decay = jnp.exp(jnp.where(causal, at - run[h : h + 1, :], -1e30))
            mats.append(decay * affinity * dt[h : h + 1, :])
        near_ref[:, cols] = near_product(mats, x_ref[:, cols].astype(F32))


def y_kernel(
    step, last, at, rows_ref, cols_ref, near_ref, x_ref, c_ref, inc_ref, in_ref, z_ref, skip_ref,
    y_ref, end_ref, sq_ref, state,
):
    @pl.when(step == 0)
    def _():
        unpack_parts(state, in_ref)

    total = rows_ref[...][:, Q - 1 :]
    grow = jnp.exp(cols_ref[:, :ROWS])
    far = far_product(c_ref[...], state[...])
    squares = jnp.zeros((Q, 2 * HEAD), F32)
    for j in range(y_ref.shape[1] // (2 * HEAD)):
        cols = pair_slice(j)
        y_pair = near_ref[:, cols] + pair_cols(grow, j) * far[:, cols]
        y_ref[:, cols] = y_pair
        after = jnp.exp(pair_row(total, j)) * state[:, cols] + inc_ref[0, :, cols]
        end_ref[0, :, cols] = after
        state[:, cols] = after
        z = z_ref[:, cols].astype(F32)
        gated = (y_pair + skip_ref[:, cols] * x_ref[:, cols].astype(F32)) * (z * sigmoid(z))
        squares += gated * gated
    row = split_mm(jnp.ones((8, 2 * HEAD), BF16), squares, NT)[:1]
    sq_ref[...] = jnp.broadcast_to(row[None], sq_ref.shape)


def token_columns(first, second):
    both = jnp.where(iota((Q, Q), 0) == 0, first, second)
    turned = jnp.transpose(both)
    return turned[:, :1], turned[:, 1:2]


def gate_kernel(
    full_width, step, last, at,
    rows_ref, c_ref, y_ref, x_ref, z_ref, g_ref, skip_ref, gain_ref, sq_ref, dot_ref,
    gy_ref, dz_ref, inc_ref, parts_ref, state,
):
    @pl.when(step == 0)
    def _():
        state[...] = jnp.zeros_like(state)

    run = rows_ref[...]
    total = run[:, Q - 1 :]
    grow = jnp.exp(run)
    c_t = jnp.transpose(c_ref[...].astype(F32))
    inverse = lax.rsqrt(jnp.sum(sq_ref[...], axis=0) / full_width + EPS)
    dots = inverse * inverse * inverse * jnp.sum(dot_ref[...], axis=0) / full_width
    inv_col, dot_col = token_columns(inverse, dots)
    for j in range(y_ref.shape[1] // (2 * HEAD)):
        cols = pair_slice(j)
        z = z_ref[:, cols].astype(F32)
        sig = sigmoid(z)
        act = z * sig
        y = y_ref[:, cols] + skip_ref[:, cols] * x_ref[:, cols].astype(F32)
        scaled = g_ref[:, cols].astype(F32) * gain_ref[:, cols]
        grad_gated = inv_col * scaled - (y * act) * dot_col
        dz_ref[:, cols] = (grad_gated * y * sig * (1.0 + z * (1.0 - sig))).astype(BF16)
        gy = (grad_gated * act).astype(BF16)
        gy_ref[:, cols] = gy
        inc = outer_state(c_t, grow, gy.astype(F32), j)
        inc_ref[0, :, cols] = inc
        state[:, cols] = jnp.exp(pair_row(total, j)) * state[:, cols] + inc

    @pl.when(last)
    def _():
        pack_parts(parts_ref, state, jnp.zeros((8, Q), F32))


def grad_near_kernel(
    step, last, at, rows_ref, cols_ref, b_ref, c_ref, gy_ref, near_ref):
    run, cols_run = rows_ref[...], cols_ref[...]
    affinity = mm(b_ref[...], c_ref[...], NT)
    later = iota((Q, Q), 1) >= iota((Q, Q), 0)
    for j in range(gy_ref.shape[1] // (2 * HEAD)):
        cols = pair_slice(j)
        mats = []
        for h in (2 * j, 2 * j + 1):
            at = jnp.broadcast_to(cols_run[:, h : h + 1], (Q, Q))
            decay = jnp.exp(jnp.where(later, run[h : h + 1, :] - at, -1e30))
            mats.append(decay * affinity)
        near_ref[:, cols] = near_product(mats, gy_ref[:, cols].astype(F32))


def grad_kernel(
    step, last, at, alog_ref, rows_ref, cols_ref, near_ref, x_ref, b_ref, y_ref, gy_ref, inc_ref, end_ref, in_ref,
    skip_ref, dx_ref, ddt_ref, state, prod,
):
    @pl.when(step == 0)
    def _():
        unpack_parts(state, in_ref)

    heads = alog_ref.shape[1]
    width = heads * HEAD
    total = rows_ref[...][:, Q - 1 :]
    cols_run = cols_ref[:, :ROWS]
    cols_dt = cols_ref[:, ROWS : 2 * ROWS]
    tail = jnp.exp(cols_run[Q - 1 :] - cols_run)
    far = far_product(b_ref[...], state[...])
    for j in range(heads // 2):
        cols = pair_slice(j)
        gy = gy_ref[:, cols].astype(F32)
        after = state[:, cols]
        grad_in = near_ref[:, cols] + pair_cols(tail, j) * far[:, cols]
        scaled = pair_cols(cols_dt, j) * grad_in
        dx_ref[:, cols] = (scaled + skip_ref[:, cols] * gy).astype(BF16)
        x = x_ref[:, cols].astype(F32)
        prod[0, :, cols] = x * grad_in
        prod[1, :, cols] = gy * y_ref[:, cols] - x * scaled
        crossing = (after * end_ref[0, :, cols]).reshape(-1, 8, 2 * HEAD)
        prod[2, :8, cols] = jnp.sum(crossing, axis=0)
        state[:, cols] = jnp.exp(pair_row(total, j)) * after + inc_ref[0, :, cols]
    heads_of = head_sum_matrix(width)
    direct = split_mm(heads_of, prod[0], NT)[:heads]
    change = split_mm(heads_of, prod[1], NT)[:heads]
    cross = jnp.sum(split_mm(heads_of, prod[2, :8, :], NT), axis=1, keepdims=True)[:heads]
    lower = (iota((Q, Q), 0) >= iota((Q, Q), 1)).astype(F32)
    grad_la = mm_exact(change, lower) + cross
    ddt_ref[...] = direct - rates(alog_ref[...]) * grad_la


def scan_kernel(reverse, own_ref, log_ref, out_ref):
    peers, rows, _ = own_ref.shape
    tiles = 2 * (rows // 8) - 1
    logs = [jnp.zeros((peers, Q), F32) for _ in range(3)]
    for k in range(peers):
        last = log_ref[k, rows - 8 :, :].astype(F32)
        for i in range(3):
            logs[i] = jnp.where(iota((peers, Q), 0) == k, last[4 + i : 5 + i, :], logs[i])
    lane = iota((Q, Q), 1)
    decays = []
    for j in range(tiles):
        pick = (iota((Q, Q), 0) == jnp.where(lane < HEAD, 2 * j, 2 * j + 1)).astype(BF16)
        decays.append(jnp.exp(sum(mm(part.astype(BF16), pick) for part in logs)))
    decays.append(jnp.ones((peers, Q), F32))
    top = iota((8, Q), 0) < 4
    for v in range(rows // 8):
        at = slice(8 * v, 8 * v + 8)
        running = jnp.zeros((8, Q), F32)
        for k in reversed(range(peers)) if reverse else range(peers):
            out_ref[k, at, :] = running.astype(BF16)
            decay = jnp.where(top, decays[2 * v][k : k + 1], decays[2 * v + 1][k : k + 1])
            running = decay * running + own_ref[k, at, :].astype(F32)


def add16(a, b):
    return (a.astype(F32) + b.astype(F32)).astype(BF16)


def params():
    return pltpu.CompilerParams(dimension_semantics=("arbitrary",))


def estimate(flops=2e9):
    return pl.CostEstimate(flops=int(flops), bytes_accessed=8 << 20, transcendentals=0)


WHOLE = object()


def index_of(cut, i):
    if cut == "rows":
        return (pl.ds(pl.multiple_of(i * Q, Q), Q), slice(None))
    if cut == "runs":
        return (pl.ds(pl.multiple_of(i * ROWS, ROWS), ROWS), slice(None))
    if cut == "cols":
        return (slice(None), pl.ds(pl.multiple_of(i * Q, Q), Q))
    if cut == "lead":
        return (pl.ds(i, 1), slice(None), slice(None))
    return (slice(None), slice(None), pl.ds(pl.multiple_of(i * Q, Q), Q))


def stream(body, blocks, reverse, ins, outs, scratch, name):
    n_in, n_out = len(ins), len(outs)

    def kernel(*refs):
        srcs, dsts = refs[:n_in], refs[n_in : n_in + n_out]
        held = refs[n_in + n_out : 2 * (n_in + n_out)]
        in_sem, out_sem = refs[2 * (n_in + n_out) : 2 * (n_in + n_out) + 2]
        rest = refs[2 * (n_in + n_out) + 2 :]
        in_held, out_held = held[:n_in], held[n_in:]

        def view(ref, cut, i):
            return ref if cut is WHOLE else ref.at[index_of(cut, i)]

        def copy_in(k, i):
            cut = ins[k][1]
            at = 0 if cut is WHOLE else i
            return pltpu.make_async_copy(
                view(srcs[k], cut, i), view(in_held[k], cut, i), in_sem.at[k, at]
            )

        def copy_out(k, i):
            cut = outs[k][1]
            at = 0 if cut is WHOLE else i
            return pltpu.make_async_copy(
                view(out_held[k], cut, i), view(dsts[k], cut, i), out_sem.at[k, at]
            )

        def place(step):
            return blocks - 1 - step if reverse else step

        for k in range(n_in):
            if ins[k][1] is WHOLE:
                copy_in(k, 0).start()

        @pl.loop(0, blocks)
        def _(step):
            for k in range(n_in):
                if ins[k][1] is not WHOLE:
                    copy_in(k, place(step)).start()

        for k in range(n_in):
            if ins[k][1] is WHOLE:
                copy_in(k, 0).wait()

        @pl.loop(0, blocks)
        def _(step):
            i = place(step)
            for k in range(n_in):
                if ins[k][1] is not WHOLE:
                    copy_in(k, i).wait()
            body(
                step, step == blocks - 1, i,
                *[view(r, cut, i) for r, (_, cut) in zip(in_held, ins)],
                *[view(r, cut, i) for r, (_, cut) in zip(out_held, outs)],
                *rest,
            )
            for k in range(n_out):
                if outs[k][1] is not WHOLE:
                    copy_out(k, i).start()

        for k in range(n_out):
            if outs[k][1] is WHOLE:
                copy_out(k, 0).start()

        @pl.loop(0, blocks)
        def _(step):
            for k in range(n_out):
                if outs[k][1] is not WHOLE:
                    copy_out(k, place(step)).wait()

        for k in range(n_out):
            if outs[k][1] is WHOLE:
                copy_out(k, 0).wait()

    anywhere = pl.BlockSpec(memory_space=pl.ANY)
    buffers = [pltpu.VMEM(v.shape, v.dtype) for v, _ in (*ins, *outs)]
    return pl.pallas_call(
        kernel,
        in_specs=[anywhere] * n_in,
        out_specs=[anywhere] * n_out,
        out_shape=[v for v, _ in outs],
        scratch_shapes=[
            *buffers,
            pltpu.SemaphoreType.DMA((n_in, blocks)),
            pltpu.SemaphoreType.DMA((n_out, blocks)),
            *scratch,
        ],
        name=name,
        compiler_params=pltpu.CompilerParams(),
        cost_estimate=estimate(),
    )(*[v for v, _ in ins])


def shards(
    x_in, z_gate, b_proj, c_proj, dt_step, a_log, skip_gain, norm_gain, out_weight, out_grad
):
    length, width = x_in.shape
    heads = a_log.shape[0]
    blocks = length // Q
    nstate = b_proj.shape[1]
    full_width = width * lax.axis_size("chan")
    alog = a_log[None]
    skip_row = jnp.repeat(skip_gain, HEAD)[None]
    gain_row = norm_gain[None]

    def shape(*dims, kind=F32):
        return jax.ShapeDtypeStruct(dims, kind)

    x_size, z_size = lax.axis_size(SEQ[0]), lax.axis_size(SEQ[1])
    peers = x_size * z_size
    x_at = lax.axis_index(SEQ[0])
    part_rows = 8 * ((heads // 2 + 1) // 2)
    parts_spec = pl.BlockSpec((peers, part_rows, Q), lambda i: (0, 0, 0))
    parts_shape = shape(peers, part_rows, Q, kind=BF16)
    wide16 = shape(length, width, kind=BF16)
    state_scratch = pltpu.VMEM((nstate, width), F32)
    chan_size = lax.axis_size("chan")
    def exchanged(parts):
        return lax.all_to_all(parts, SEQ, 0, 0, tiled=True)

    def scanned(own, logs, reverse, name):
        return pl.pallas_call(
            functools.partial(scan_kernel, reverse),
            grid=(1,),
            in_specs=[parts_spec, parts_spec],
            out_specs=parts_spec,
            out_shape=parts_shape,
            name=name,
            compiler_params=params(),
            cost_estimate=estimate(),
        )(own, logs)

    def everyones(copies):
        return lax.all_to_all(copies, "chan", 0, 0, tiled=True)

    def shifted(value, by):
        return lax.ppermute(value, SEQ[0], [(i, (i + by) % x_size) for i in range(x_size)])

    slots = [out_weight] + [shifted(out_weight, -k) for k in range(1, x_size)]

    states = shape(blocks, nstate, width)
    inc, own_parts, run_rows, run_cols = stream(
        functools.partial(state_kernel, blocks),
        blocks, False,
        [(dt_step, WHOLE), (alog, WHOLE), (x_in, "rows"), (b_proj, "rows")],
        [(states, "lead"), (parts_shape, WHOLE), (shape(ROWS * blocks, Q), WHOLE),
         (shape(length, Q), WHOLE)],
        [state_scratch, pltpu.VMEM((ROWS, Q), F32)],
        "own_state",
    )
    *slots, own_parts = lax.optimization_barrier((*slots, own_parts))
    logs = exchanged(own_parts)
    stacked, logs = lax.optimization_barrier((jnp.stack(slots), logs))
    weight = lax.all_gather(stacked, SEQ[1])

    near, = stream(
        near_kernel, blocks, False,
        [(dt_step, "cols"), (run_rows, "runs"), (run_cols, "rows"), (x_in, "rows"),
         (b_proj, "rows"), (c_proj, "rows")],
        [(shape(length, width), "rows")], [], "near",
    )
    state_in = exchanged(scanned(logs, logs, False, "scan_up"))

    y, ends, squares = stream(
        y_kernel, blocks, False,
        [(run_rows, "runs"), (run_cols, "rows"), (near, "rows"), (x_in, "rows"),
         (c_proj, "rows"), (inc, "lead"), (state_in, WHOLE), (z_gate, "rows"),
         (skip_row, WHOLE)],
        [(shape(length, width), "rows"), (states, "lead"),
         (shape(chan_size, 1, length), "last")],
        [state_scratch], "y",
    )
    all_squares = everyones(squares)

    z_vals = z_gate.astype(F32)
    gated = (y + skip_row * x_in.astype(F32)) * (z_vals * sigmoid(z_vals))

    inverse = lax.rsqrt(jnp.sum(all_squares, axis=(0, 1)) / full_width + EPS)
    normed = (gated * inverse[:, None] * gain_row).astype(BF16)
    normed = lax.optimization_barrier(normed)
    block_rows = out_grad.shape[1] // x_size

    def outer(at):
        block = lax.dynamic_slice_in_dim(out_grad, (at % x_size) * block_rows, block_rows, 1)
        return lax.dot_general(
            block, normed, (((0,), (0,)), ((), ())), preferred_element_type=F32
        ).astype(BF16)

    half = block_rows // 2
    far = outer(x_at + 2)
    far_up = shifted(far[:half], 1)
    far_down = shifted(far[half:], -1)
    far, weight = lax.optimization_barrier((far, weight))

    order = (jnp.arange(x_size) - x_at) % x_size
    weight = jnp.swapaxes(weight, 0, 1)[order].reshape(-1, width)
    grad_norm = mm(out_grad, weight).astype(BF16)
    dots = jnp.sum(gated * (grad_norm.astype(F32) * gain_row), axis=1)
    all_dots = everyones(jnp.broadcast_to(dots[None, None], (chan_size, 1, length)))

    right, left, held = outer(x_at + 1), outer(x_at + x_size - 1), outer(x_at)
    far_up, far_down, grad_norm = lax.optimization_barrier((far_up, far_down, grad_norm))
    right = jnp.concatenate([add16(right[:half], far_up), right[half:]], axis=0)
    left = jnp.concatenate([left[:half], add16(left[half:], far_down)], axis=0)
    from_left, from_right = shifted(right, 1), shifted(left, -1)

    grad_y, grad_z, grad_inc, own_grad = stream(
        functools.partial(gate_kernel, float(full_width)),
        blocks, True,
        [(run_rows, "runs"), (c_proj, "rows"), (y, "rows"), (x_in, "rows"), (z_gate, "rows"),
         (grad_norm, "rows"), (skip_row, WHOLE), (gain_row, WHOLE), (all_squares, "last"),
         (all_dots, "last")],
        [(wide16, "rows"), (wide16, "rows"), (states, "lead"), (parts_shape, WHOLE)],
        [state_scratch], "gate",
    )
    from_left, from_right, own_grad = lax.optimization_barrier((from_left, from_right, own_grad))
    held = held.astype(F32) + from_left.astype(F32) + from_right.astype(F32)
    weight_grad = lax.psum_scatter(held, SEQ[1], scatter_dimension=0, tiled=True)
    near, = stream(
        grad_near_kernel, blocks, False,
        [(run_rows, "runs"), (run_cols, "rows"), (b_proj, "rows"), (c_proj, "rows"),
         (grad_y, "rows")],
        [(shape(length, width), "rows")], [], "grad_near",
    )
    grad_out = exchanged(scanned(exchanged(own_grad), logs, True, "scan_down"))
    grad_x, grad_dt = stream(
        grad_kernel, blocks, True,
        [(alog, WHOLE), (run_rows, "runs"), (run_cols, "rows"), (near, "rows"), (x_in, "rows"),
         (b_proj, "rows"), (y, "rows"), (grad_y, "rows"), (grad_inc, "lead"), (ends, "lead"),
         (grad_out, WHOLE), (skip_row, WHOLE)],
        [(wide16, "rows"), (shape(heads, length), "cols")],
        [state_scratch, pltpu.VMEM((3, Q, width), F32)], "grad",
    )
    return (grad_x, grad_z, grad_dt, weight_grad)


def solution(mesh):
    z_axis = 8 if mesh.shape["seq"] % 8 == 0 else 1
    torus = Mesh(
        mesh.devices.reshape(-1, z_axis, mesh.shape["chan"]), ("seq_0", "seq_1", "chan")
    )
    return jax.shard_map(
        shards,
        mesh=torus,
        in_specs=(
            P(SEQ, "chan"),
            P(SEQ, "chan"),
            P(SEQ, None),
            P(SEQ, None),
            P("chan", SEQ),
            P("chan"),
            P("chan"),
            P("chan"),
            P(SEQ, "chan"),
            P(SEQ, None),
        ),
        out_specs=(P(SEQ, "chan"), P(SEQ, "chan"), P("chan", SEQ), P(SEQ, "chan")),
        check_vma=False,
    )
```
